32 devices in a mesh: row: 4 (over y, x), col: 8 (over z, core).
Axes of the slice: x: 2, y: 2, z: 4, core: 2. Of those that a mesh axis runs over, the one named last changes fastest.
Arguments:
- view_a: bfloat16 [3072, 8192], P(('row', 'col')), may hold values from -1000 to 1000
- view_b: bfloat16 [3072, 8192], P(('row', 'col')), may hold values from -1000 to 1000
Outputs:
- correlation: float32 [8192, 8192], P('row', 'col')
- loss: float32 [], replicated
The draws below stay inside these ranges and needn't reach their ends.
All inputs are finite; a program needn't handle non-finite values.
Results may differ from the reference program's by a relative error of at most 0.0013.
Values may be sent and summed in bfloat16 or wider, within the bound.
A program may use at most 192 MiB of HBM per device.

```python
import jax
import jax.numpy as jnp
from jax import lax

D = 8192
TOKENS = 3072


def draw_pair(key):
    keys = jax.random.split(jax.random.fold_in(key, 11), 6)
    ramp = jnp.arange(TOKENS, dtype=jnp.float32) / max(TOKENS - 1, 1)
    row_scale = (1.0 + 2.0 * ramp) * jnp.exp(jax.random.uniform(keys[0], (TOKENS,), jnp.float32, 0.0, jnp.log(3.0)))
    col_scale = jnp.exp(jax.random.uniform(keys[1], (D,), jnp.float32, 0.0, jnp.log(10.0)))
    mixing = jax.random.uniform(keys[2], (D,), jnp.float32, 0.2, 0.95)
    offset = 0.5 * jax.random.normal(keys[3], (D,), jnp.float32)
    base = jax.random.normal(keys[4], (TOKENS, D), jnp.float32)
    noise = jax.random.normal(keys[5], (TOKENS, D), jnp.float32)
    other = mixing * base + jnp.sqrt(1.0 - mixing * mixing) * noise
    scale = row_scale[:, None] * col_scale[None, :]
    first = jnp.clip((base + offset) * scale, -1000.0, 1000.0)
    second = jnp.clip((other + offset) * scale, -1000.0, 1000.0)
    return (first, second)


def draw_view_a(key, part):
    return draw_pair(key)[0].astype(jnp.bfloat16)


def draw_view_b(key, part):
    return draw_pair(key)[1].astype(jnp.bfloat16)


def setup_inputs(seed: int = 0) -> dict:
    seeds = jax.random.split(jax.random.key(seed), 3)
    return {
        "view_a": draw_view_a(jax.random.fold_in(seeds[2], 71), 0),
        "view_b": draw_view_b(jax.random.fold_in(seeds[2], 71), 0),
    }


def normalize(view):
    values = view.astype(jnp.float32)
    count = view.shape[0]
    mean = lax.optimization_barrier(jnp.sum(values, 0)) / count
    var = lax.optimization_barrier(jnp.sum(values * values, 0)) / count - mean * mean
    return ((values - mean) * lax.rsqrt(var + 1e-05)).astype(jnp.bfloat16)

def reference(view_a, view_b):
    norm_a = normalize(view_a).astype(jnp.float32)
    norm_b = normalize(view_b).astype(jnp.float32)
    product = lax.dot_general(norm_a, norm_b, (((0,), (0,)), ((), ())), precision=lax.Precision.HIGHEST, preferred_element_type=jnp.float32)
    correlation = product / view_a.shape[0]
    diag = jnp.diagonal(correlation)
    total = 0.0051 * jnp.sum(correlation * correlation) + jnp.sum((1.0 - diag) ** 2 - 0.0051 * diag * diag)
    loss = total / view_a.shape[1]
    return (correlation, loss)
```

```python
import functools

import jax
import jax.numpy as jnp
from jax import lax
from jax.experimental import pallas as pl
from jax.experimental.pallas import tpu as pltpu
from jax.sharding import PartitionSpec as P

MESH = pl.DeviceIdType.MESH
F32 = jnp.float32
BF16 = jnp.bfloat16


def body(
    n_row, n_col, width,
    a_in, b_in, out, loss_out,
    a_all, b_all, nb, stat_a, stat_b, coef_a, coef_b, loss_row, loss_col,
    s_a, r_a, s_b, r_b, s_sa, r_sa, s_sb, r_sb, s_line, r_line, s_fwd, r_fwd,
    s_lr, r_lr, s_lc, r_lc, own_sem,
):
    t = a_in.shape[0]
    rb = a_in.shape[1] // n_row
    cb = b_in.shape[1] // n_col
    count = t * n_row * n_col
    n_z = n_col // 2
    r = lax.axis_index("row")
    c = lax.axis_index("col")
    z = c // 2
    k = c % 2
    mine = pl.ds(pl.multiple_of(r * t, t), t)

    def row_mate(i):
        return (r + i) % n_row

    def col_mate(j):
        return (c + j) % n_col

    def remote(src, dst, ss, rs, dev):
        return pltpu.make_async_remote_copy(
            src_ref=src, dst_ref=dst, send_sem=ss, recv_sem=rs, device_id=dev, device_id_type=MESH
        )

    barrier = pltpu.get_barrier_semaphore()
    for i in range(1, n_row):
        pl.semaphore_signal(barrier, inc=1, device_id=(row_mate(i), c), device_id_type=MESH)
    for j in range(1, n_col):
        pl.semaphore_signal(barrier, inc=1, device_id=(r, col_mate(j)), device_id_type=MESH)
    pl.semaphore_wait(barrier, n_row + n_col - 2)

    def send_a(i):
        dst = row_mate(i)
        cols = pl.ds(pl.multiple_of(dst * rb, rb), rb)
        return remote(a_in.at[:, cols], a_all.at[c, mine], s_a.at[i], r_a.at[i], (dst, c))

    def got_a(i):
        src = row_mate(n_row - i)
        rows = pl.ds(pl.multiple_of(src * t, t), t)
        return remote(a_all.at[c, rows], a_all.at[c, rows], s_a.at[i], r_a.at[i], (src, c))

    def send_b(j):
        dst = col_mate(j)
        cols = pl.ds(pl.multiple_of(dst * cb, cb), cb)
        return remote(b_in.at[:, cols], b_all.at[c, mine], s_b.at[j], r_b.at[j], (r, dst))

    def got_b(j):
        src = col_mate(n_col - j)
        return remote(b_all.at[src, mine], b_all.at[src, mine], s_b.at[j], r_b.at[j], (r, src))

    for i in range(1, n_row):
        send_a(i).start()
    for j in range(1, n_col):
        send_b(j).start()
    own_a = pltpu.make_async_copy(
        a_in.at[:, pl.ds(pl.multiple_of(r * rb, rb), rb)], a_all.at[c, mine], own_sem.at[0]
    )
    own_b = pltpu.make_async_copy(
        b_in.at[:, pl.ds(pl.multiple_of(c * cb, cb), cb)], b_all.at[c, mine], own_sem.at[1]
    )
    own_a.start()
    own_b.start()

    own_a.wait()
    for i in range(1, n_row):
        got_a(i).wait_recv()

    def moments_a(q, carry):
        cols = pl.ds(pl.multiple_of(q * 128, 128), 128)
        x = a_all[c, :, cols].astype(F32)
        stat_a[c, 0:1, cols] = jnp.sum(x, 0, keepdims=True)
        stat_a[c, 1:2, cols] = jnp.sum(x * x, 0, keepdims=True)
        return carry

    lax.fori_loop(0, rb // 128, moments_a, 0)

    def send_sa(j):
        return remote(stat_a.at[c], stat_a.at[c], s_sa.at[j], r_sa.at[j], (r, col_mate(j)))

    def got_sa(j):
        src = col_mate(n_col - j)
        return remote(stat_a.at[src], stat_a.at[src], s_sa.at[j], r_sa.at[j], (r, src))

    for j in range(1, n_col):
        send_sa(j).start()

    def line(way, chunk, p, dev_c):
        rows = pl.ds(pl.multiple_of(p * t, t), t)
        ref = a_all.at[chunk, rows]
        return remote(ref, ref, s_line.at[way, chunk, p], r_line.at[chunk, p], (r, dev_c))

    partner = z * 2 + (1 - k)

    def up(chunk, p):
        return line(0, chunk, p, lax.min(c + 2, n_col - 2 + k))

    def down(chunk, p):
        return line(1, chunk, p, lax.max(c - 2, k))

    def across(chunk, p):
        return line(2, chunk, p, partner)

    can_up = z < n_z - 1
    can_down = z > 0

    for p in range(n_row):
        @pl.when(can_up)
        def _():
            up(c, p).start()

        @pl.when(can_down)
        def _():
            down(c, p).start()

        across(c, p).start()

    own_b.wait()
    for j in range(1, n_col):
        got_b(j).wait_recv()

    def moments_b(q, carry):
        cols = pl.ds(pl.multiple_of(q * 128, 128), 128)
        total = jnp.zeros((1, 128), F32)
        squares = jnp.zeros((1, 128), F32)
        for g in range(n_col):
            x = b_all[g, mine, cols].astype(F32)
            total = total + jnp.sum(x, 0, keepdims=True)
            squares = squares + jnp.sum(x * x, 0, keepdims=True)
        stat_b[r, 0:1, cols] = total
        stat_b[r, 1:2, cols] = squares
        return carry

    lax.fori_loop(0, cb // 128, moments_b, 0)

    def send_sb(i):
        return remote(stat_b.at[r], stat_b.at[r], s_sb.at[i], r_sb.at[i], (row_mate(i), c))

    def got_sb(i):
        src = row_mate(n_row - i)
        return remote(stat_b.at[src], stat_b.at[src], s_sb.at[i], r_sb.at[i], (src, c))

    for i in range(1, n_row):
        send_sb(i).start()

    def send_fwd(i, g):
        return remote(b_all.at[g, mine], b_all.at[g, mine], s_fwd.at[i, g], r_fwd.at[i, g], (row_mate(i), c))

    def got_fwd(i, g):
        src = row_mate(n_row - i)
        rows = pl.ds(pl.multiple_of(src * t, t), t)
        return remote(b_all.at[g, rows], b_all.at[g, rows], s_fwd.at[i, g], r_fwd.at[i, g], (src, c))

    def each_chunk(d, do):
        for side in range(2):
            zz = z - d if side == 0 else z + d
            ok = (zz >= 0) if side == 0 else jnp.logical_and(zz < n_z, d > 0)

            @pl.when(ok)
            def _():
                do(zz * 2 + k, side)
                do(zz * 2 + (1 - k), side)

    def forward(d, carry):
        def do(g, side):
            for i in range(1, n_row):
                send_fwd(i, g).start()

        each_chunk(d, do)
        return carry

    lax.fori_loop(0, n_z, forward, 0)

    def clear(q, carry):
        rows = pl.ds(pl.multiple_of(q * 64, 64), 64)
        out[rows, :] = jnp.zeros((64, cb), F32)
        return carry

    lax.fori_loop(0, rb // 64, clear, 0)

    for j in range(1, n_col):
        got_sa(j).wait_recv()
    for i in range(1, n_row):
        got_sb(i).wait_recv()

    def coefs(stat, coef):
        sums = jnp.sum(stat[...], 0)
        mean = sums[0:1] / count
        var = sums[1:2] / count - mean * mean
        coef[0:1, :] = mean
        coef[1:2, :] = lax.rsqrt(var + 1e-05)

    coefs(stat_a, coef_a)
    coefs(stat_b, coef_b)

    tile = 256

    def process(g, side):
        for i in range(1, n_row):
            got_fwd(i, g).wait_recv()

        def norm_b(q, carry):
            cols = pl.ds(pl.multiple_of(q * 128, 128), 128)
            x = b_all[g, :, cols].astype(F32)
            nb[:, cols] = ((x - coef_b[0:1, cols]) * coef_b[1:2, cols]).astype(BF16)
            return carry

        lax.fori_loop(0, cb // 128, norm_b, 0)

        def mul(q, carry):
            cols = pl.ds(pl.multiple_of(q * tile, tile), tile)
            x = a_all[g, :, cols].astype(F32)
            na = ((x - coef_a[0:1, cols]) * coef_a[1:2, cols]).astype(BF16)
            out[cols, :] += lax.dot_general(
                na, nb[...], (((0,), (0,)), ((), ())), preferred_element_type=F32
            )
            return carry

        lax.fori_loop(0, rb // tile, mul, 0)

    def process_all(d):
        def one(q, carry):
            side = q // 2
            zz = jnp.where(side == 0, z - d, z + d)
            ok = jnp.logical_and(zz >= 0, zz < n_z)
            ok = jnp.logical_and(ok, jnp.logical_or(side == 0, d > 0))
            other = q % 2
            g = zz * 2 + jnp.where(other == 0, k, 1 - k)

            @pl.when(ok)
            def _():
                @pl.when(other == 1)
                def _():
                    for p in range(n_row):
                        across(g, p).wait_recv()

                process(g, 0)

            return carry

        lax.fori_loop(0, 4, one, 0)

    def step(d, carry):
        from_low = z - d >= 0
        from_high = z + d < n_z
        low = (z - d) * 2 + k
        high = (z + d) * 2 + k
        for p in range(n_row):
            @pl.when(from_low)
            def _():
                up(low, p).wait_recv()

                @pl.when(can_up)
                def _():
                    up(low, p).start()

                across(low, p).start()

            @pl.when(from_high)
            def _():
                down(high, p).wait_recv()

                @pl.when(can_down)
                def _():
                    down(high, p).start()

                across(high, p).start()

        process_all(d - 1)
        return carry

    lax.fori_loop(1, n_z, step, 0)
    process_all(n_z - 1)

    def part(q, carry):
        rows = pl.ds(pl.multiple_of(q * 8, 8), 8)
        x = out[rows, :] / count
        row_ids = r * rb + q * 8 + lax.broadcasted_iota(jnp.int32, (8, cb), 0)
        col_ids = c * cb + lax.broadcasted_iota(jnp.int32, (8, cb), 1)
        sq = x * x
        return carry + jnp.where(row_ids == col_ids, (1.0 - x) * (1.0 - x), 0.0051 * sq)

    share = lax.fori_loop(0, rb // 8, part, jnp.zeros((8, cb), F32), unroll=4)
    folded = share[:, 0:128]
    for q in range(1, cb // 128):
        folded = folded + share[:, q * 128 : (q + 1) * 128]
    loss_row[r] = folded

    def send_lr(i):
        return remote(loss_row.at[r], loss_row.at[r], s_lr.at[i], r_lr.at[i], (row_mate(i), c))

    def got_lr(i):
        src = row_mate(n_row - i)
        return remote(loss_row.at[src], loss_row.at[src], s_lr.at[i], r_lr.at[i], (src, c))

    def send_lc(j):
        return remote(loss_col.at[c], loss_col.at[c], s_lc.at[j], r_lc.at[j], (r, col_mate(j)))

    def got_lc(j):
        src = col_mate(n_col - j)
        return remote(loss_col.at[src], loss_col.at[src], s_lc.at[j], r_lc.at[j], (r, src))

    for i in range(1, n_row):
        send_lr(i).start()
    for i in range(1, n_row):
        got_lr(i).wait_recv()
    loss_col[c] = jnp.sum(loss_row[...], 0)
    for j in range(1, n_col):
        send_lc(j).start()

    for i in range(1, n_row):
        send_a(i).wait_send()
        send_sb(i).wait_send()
        send_lr(i).wait_send()
    for j in range(1, n_col):
        send_b(j).wait_send()
        send_sa(j).wait_send()

    def drain(g, carry):
        for i in range(1, n_row):
            send_fwd(i, g).wait_send()
        zz = g // 2
        for p in range(n_row):
            @pl.when(g % 2 == k)
            def _():
                @pl.when(jnp.logical_and(zz <= z, can_up))
                def _():
                    up(g, p).wait_send()

                @pl.when(jnp.logical_and(zz >= z, can_down))
                def _():
                    down(g, p).wait_send()

                across(g, p).wait_send()

        return carry

    lax.fori_loop(0, n_col, drain, 0)

    for j in range(1, n_col):
        got_lc(j).wait_recv()
    loss_out[...] = jnp.broadcast_to(
        jnp.sum(jnp.sum(loss_col[...], 0), keepdims=True) / width, loss_out.shape
    )
    for j in range(1, n_col):
        send_lc(j).wait_send()


def shards(view_a, view_b):
    t, width = view_a.shape
    n_row = lax.axis_size("row")
    n_col = lax.axis_size("col")
    rb = width // n_row
    cb = width // n_col
    count = t * n_row * n_col
    n_chunk = t * n_row
    dma = pltpu.SemaphoreType.DMA
    size = 2 * (count * (rb + cb) + n_chunk * cb + 2 * t * width) + 4 * rb * cb
    product, loss = pl.pallas_call(
        functools.partial(body, n_row, n_col, width),
        out_shape=(
            jax.ShapeDtypeStruct((rb, cb), F32),
            jax.ShapeDtypeStruct((8, 128), F32),
        ),
        in_specs=[pl.BlockSpec(memory_space=pltpu.VMEM)] * 2,
        out_specs=(pl.BlockSpec(memory_space=pltpu.VMEM),) * 2,
        scratch_shapes=[
            pltpu.VMEM((n_col, n_chunk, rb), BF16),
            pltpu.VMEM((n_col, n_chunk, cb), BF16),
            pltpu.VMEM((n_chunk, cb), BF16),
            pltpu.VMEM((n_col, 2, rb), F32),
            pltpu.VMEM((n_row, 2, cb), F32),
            pltpu.VMEM((2, rb), F32),
            pltpu.VMEM((2, cb), F32),
            pltpu.VMEM((n_row, 8, 128), F32),
            pltpu.VMEM((n_col, 8, 128), F32),
            dma((n_row,)), dma((n_row,)),
            dma((n_col,)), dma((n_col,)),
            dma((n_col,)), dma((n_col,)),
            dma((n_row,)), dma((n_row,)),
            dma((3, n_col, n_row)), dma((n_col, n_row)),
            dma((n_row, n_col)), dma((n_row, n_col)),
            dma((n_row,)), dma((n_row,)),
            dma((n_col,)), dma((n_col,)),
            dma((2,)),
        ],
        compiler_params=pltpu.CompilerParams(
            collective_id=0, has_side_effects=True, vmem_limit_bytes=size + (4 << 20)
        ),
        name="twins",
    )(view_a, view_b)
    return product / count, loss[0, 0]


def solution(mesh):
    return jax.shard_map(
        shards,
        mesh=mesh,
        in_specs=(P(("row", "col"), None), P(("row", "col"), None)),
        out_specs=(P("row", "col"), P()),
        check_vma=False,
    )
```

```python
import functools

import jax
import jax.numpy as jnp
from jax import lax
from jax.experimental import pallas as pl
from jax.experimental.pallas import tpu as pltpu
from jax.sharding import PartitionSpec as P

MESH = pl.DeviceIdType.MESH
F32 = jnp.float32
BF16 = jnp.bfloat16


def body(
    n_row, n_col, width,
    a_in, b_in, out, loss_out,
    a_all, b_all, nb, stat_a, stat_b, coef_a, coef_b, loss_row, loss_col,
    s_a, r_a, s_b, r_b, s_sa, r_sa, s_sb, r_sb, s_line, r_line, s_fwd, r_fwd,
    s_lr, r_lr, s_lc, r_lc, own_sem,
):
    t = a_in.shape[0]
    rb = a_in.shape[1] // n_row
    cb = b_in.shape[1] // n_col
    count = t * n_row * n_col
    n_z = n_col // 2
    r = lax.axis_index("row")
    c = lax.axis_index("col")
    z = c // 2
    k = c % 2
    mine = pl.ds(pl.multiple_of(r * t, t), t)

    def row_mate(i):
        return (r + i) % n_row

    def col_mate(j):
        return (c + j) % n_col

    def remote(src, dst, ss, rs, dev):
        return pltpu.make_async_remote_copy(
            src_ref=src, dst_ref=dst, send_sem=ss, recv_sem=rs, device_id=dev, device_id_type=MESH
        )

    own_a = pltpu.make_async_copy(
        a_in.at[:, pl.ds(pl.multiple_of(r * rb, rb), rb)], a_all.at[c, mine], own_sem.at[0]
    )
    own_b = pltpu.make_async_copy(
        b_in.at[:, pl.ds(pl.multiple_of(c * cb, cb), cb)], b_all.at[c, mine], own_sem.at[1]
    )
    own_a.start()
    own_b.start()

    barrier = pltpu.get_barrier_semaphore()
    for i in range(1, n_row):
        pl.semaphore_signal(barrier, inc=1, device_id=(row_mate(i), c), device_id_type=MESH)
    for j in range(1, n_col):
        pl.semaphore_signal(barrier, inc=1, device_id=(r, col_mate(j)), device_id_type=MESH)
    pl.semaphore_wait(barrier, n_row + n_col - 2)

    def send_a(i):
        dst = row_mate(i)
        cols = pl.ds(pl.multiple_of(dst * rb, rb), rb)
        return remote(a_in.at[:, cols], a_all.at[c, mine], s_a.at[i], r_a.at[i], (dst, c))

    def got_a(i):
        src = row_mate(n_row - i)
        rows = pl.ds(pl.multiple_of(src * t, t), t)
        return remote(a_all.at[c, rows], a_all.at[c, rows], s_a.at[i], r_a.at[i], (src, c))

    def send_b(j):
        dst = col_mate(j)
        cols = pl.ds(pl.multiple_of(dst * cb, cb), cb)
        return remote(b_in.at[:, cols], b_all.at[c, mine], s_b.at[j], r_b.at[j], (r, dst))

    def got_b(j):
        src = col_mate(n_col - j)
        return remote(b_all.at[src, mine], b_all.at[src, mine], s_b.at[j], r_b.at[j], (r, src))

    for i in range(1, n_row):
        send_a(i).start()

    def line(way, chunk, p, dev_c):
        rows = pl.ds(pl.multiple_of(p * t, t), t)
        ref = a_all.at[chunk, rows]
        return remote(ref, ref, s_line.at[way, chunk, p], r_line.at[chunk, p], (r, dev_c))

    partner = z * 2 + (1 - k)

    def up(chunk, p):
        return line(0, chunk, p, lax.min(c + 2, n_col - 2 + k))

    def down(chunk, p):
        return line(1, chunk, p, lax.max(c - 2, k))

    def across(chunk, p):
        return line(2, chunk, p, partner)

    can_up = z < n_z - 1
    can_down = z > 0

    def slice_at(o):
        return (r + n_row - o) % n_row

    def send_line(o):
        p = slice_at(o)

        @pl.when(can_up)
        def _():
            up(c, p).start()

        @pl.when(can_down)
        def _():
            down(c, p).start()

        across(c, p).start()

    own_a.wait()
    send_line(0)

    for dist in range(n_z - 1, 0, -1):
        for side in range(2):
            zz = z - dist if side == 0 else z + dist

            @pl.when(jnp.logical_and(zz >= 0, zz < n_z))
            def _():
                for other in range(2):
                    send_b((zz * 2 + (k + other) % 2 + n_col - c) % n_col).start()

    send_b((partner + n_col - c) % n_col).start()

    for o in range(1, n_row):
        got_a(o).wait_recv()
        if o < n_row - 1:
            send_line(o)

    def moments_a(q, carry):
        cols = pl.ds(pl.multiple_of(q * 128, 128), 128)
        x = a_all[c, :, cols].astype(F32)
        stat_a[c, 0:1, cols] = jnp.sum(x, 0, keepdims=True)
        stat_a[c, 1:2, cols] = jnp.sum(x * x, 0, keepdims=True)
        return carry

    lax.fori_loop(0, rb // 128, moments_a, 0)

    def send_sa(j):
        return remote(stat_a.at[c], stat_a.at[c], s_sa.at[j], r_sa.at[j], (r, col_mate(j)))

    def got_sa(j):
        src = col_mate(n_col - j)
        return remote(stat_a.at[src], stat_a.at[src], s_sa.at[j], r_sa.at[j], (r, src))

    for j in range(1, n_col):
        send_sa(j).start()
    if n_row > 1:
        send_line(n_row - 1)

    def send_fwd(i, g):
        return remote(b_all.at[g, mine], b_all.at[g, mine], s_fwd.at[i, g], r_fwd.at[i, g], (row_mate(i), c))

    def got_fwd(i, g):
        src = row_mate(n_row - i)
        rows = pl.ds(pl.multiple_of(src * t, t), t)
        return remote(b_all.at[g, rows], b_all.at[g, rows], s_fwd.at[i, g], r_fwd.at[i, g], (src, c))

    def each_chunk(d, do):
        for side in range(2):
            zz = z - d if side == 0 else z + d
            ok = (zz >= 0) if side == 0 else jnp.logical_and(zz < n_z, d > 0)

            @pl.when(ok)
            def _():
                do(zz * 2 + k, side)
                do(zz * 2 + (1 - k), side)

    def forward(d, carry):
        def do(g, side):
            for i in range(1, n_row):
                send_fwd(i, g).start()

        each_chunk(d, do)
        return carry

    own_b.wait()
    near = 1 + (n_col - 2) * (1 - k)
    got_b(near).wait_recv()
    forward(0, 0)
    for j in range(1, n_col):
        @pl.when(j != near)
        def _():
            got_b(j).wait_recv()


    def moments_b(q, carry):
        cols = pl.ds(pl.multiple_of(q * 128, 128), 128)
        total = jnp.zeros((1, 128), F32)
        squares = jnp.zeros((1, 128), F32)
        for g in range(n_col):
            x = b_all[g, mine, cols].astype(F32)
            total = total + jnp.sum(x, 0, keepdims=True)
            squares = squares + jnp.sum(x * x, 0, keepdims=True)
        stat_b[r, 0:1, cols] = total
        stat_b[r, 1:2, cols] = squares
        return carry

    lax.fori_loop(0, cb // 128, moments_b, 0)

    def send_sb(i):
        return remote(stat_b.at[r], stat_b.at[r], s_sb.at[i], r_sb.at[i], (row_mate(i), c))

    def got_sb(i):
        src = row_mate(n_row - i)
        return remote(stat_b.at[src], stat_b.at[src], s_sb.at[i], r_sb.at[i], (src, c))

    for i in range(1, n_row):
        send_sb(i).start()

    lax.fori_loop(1, n_z, forward, 0)

    def clear(q, carry):
        rows = pl.ds(pl.multiple_of(q * 64, 64), 64)
        out[rows, :] = jnp.zeros((64, cb), F32)
        return carry

    lax.fori_loop(0, rb // 64, clear, 0)

    for j in range(1, n_col):
        got_sa(j).wait_recv()
    for i in range(1, n_row):
        got_sb(i).wait_recv()

    def coefs(stat, coef):
        sums = jnp.sum(stat[...], 0)
        mean = sums[0:1] / count
        var = sums[1:2] / count - mean * mean
        coef[0:1, :] = mean
        coef[1:2, :] = lax.rsqrt(var + 1e-05)

    coefs(stat_a, coef_a)
    coefs(stat_b, coef_b)

    tile = min(1024, rb)
    depth = 2 * n_row * t

    def process(zz):
        pair = pl.ds(zz * 2, 2)
        for p in range(n_row):
            across(zz * 2 + (1 - k), p).wait_recv()
        for g in range(2):
            for i in range(1, n_row):
                got_fwd(i, zz * 2 + g).wait_recv()

        def norm_b(q, carry):
            cols = pl.ds(pl.multiple_of(q * 128, 128), 128)
            x = b_all[pair, :, cols].astype(F32).reshape(depth, 128)
            nb[:, cols] = ((x - coef_b[0:1, cols]) * coef_b[1:2, cols]).astype(BF16)
            return carry

        lax.fori_loop(0, cb // 128, norm_b, 0)

        def mul(q, carry):
            cols = pl.ds(pl.multiple_of(q * tile, tile), tile)
            x = a_all[pair, :, cols].astype(F32).reshape(depth, tile)
            na = ((x - coef_a[0:1, cols]) * coef_a[1:2, cols]).astype(BF16)
            out[cols, :] += lax.dot_general(
                na, nb[...], (((0,), (0,)), ((), ())), preferred_element_type=F32
            )
            return carry

        lax.fori_loop(0, rb // tile, mul, 0)

    def process_all(d):
        def one(side, carry):
            zz = jnp.where(side == 0, z - d, z + d)
            ok = jnp.logical_and(zz >= 0, zz < n_z)
            ok = jnp.logical_and(ok, jnp.logical_or(side == 0, d > 0))

            @pl.when(ok)
            def _():
                process(zz)

            return carry

        lax.fori_loop(0, 2, one, 0)

    def relay(d):
        from_low = z - d >= 0
        from_high = z + d < n_z
        low = (z - d) * 2 + k
        high = (z + d) * 2 + k
        for o in range(n_row):
            p = slice_at(o)

            @pl.when(from_low)
            def _():
                up(low, p).wait_recv()

                @pl.when(can_up)
                def _():
                    up(low, p).start()

                across(low, p).start()

            @pl.when(from_high)
            def _():
                down(high, p).wait_recv()

                @pl.when(can_down)
                def _():
                    down(high, p).start()

                across(high, p).start()

    def step(d, carry):
        @pl.when(d + 1 < n_z - 1)
        def _():
            relay(d + 1)

        process_all(d)

        @pl.when(d + 1 == n_z - 1)
        def _():
            relay(d + 1)

        return carry

    lax.fori_loop(0, n_z, step, 0)

    def part(q, carry):
        rows = pl.ds(pl.multiple_of(q * 8, 8), 8)
        x = out[rows, :] * (1.0 / count)
        row_ids = r * rb + q * 8 + lax.broadcasted_iota(jnp.int32, (8, cb), 0)
        col_ids = c * cb + lax.broadcasted_iota(jnp.int32, (8, cb), 1)
        sq = x * x
        return carry + jnp.where(row_ids == col_ids, (1.0 - x) * (1.0 - x), 0.0051 * sq)

    share = lax.fori_loop(0, rb // 8, part, jnp.zeros((8, cb), F32), unroll=4)
    folded = share[:, 0:128]
    for q in range(1, cb // 128):
        folded = folded + share[:, q * 128 : (q + 1) * 128]
    loss_row[r] = folded

    def send_lr(i):
        return remote(loss_row.at[r], loss_row.at[r], s_lr.at[i], r_lr.at[i], (row_mate(i), c))

    def got_lr(i):
        src = row_mate(n_row - i)
        return remote(loss_row.at[src], loss_row.at[src], s_lr.at[i], r_lr.at[i], (src, c))

    def send_lc(j):
        return remote(loss_col.at[c], loss_col.at[c], s_lc.at[j], r_lc.at[j], (r, col_mate(j)))

    def got_lc(j):
        src = col_mate(n_col - j)
        return remote(loss_col.at[src], loss_col.at[src], s_lc.at[j], r_lc.at[j], (r, src))

    for i in range(1, n_row):
        send_lr(i).start()
    for i in range(1, n_row):
        got_lr(i).wait_recv()
    loss_col[c] = jnp.sum(loss_row[...], 0)
    for j in range(1, n_col):
        send_lc(j).start()

    for i in range(1, n_row):
        send_a(i).wait_send()
        send_sb(i).wait_send()
        send_lr(i).wait_send()
    for j in range(1, n_col):
        send_b(j).wait_send()
        send_sa(j).wait_send()

    def drain(g, carry):
        for i in range(1, n_row):
            send_fwd(i, g).wait_send()
        zz = g // 2
        for p in range(n_row):
            @pl.when(g % 2 == k)
            def _():
                @pl.when(jnp.logical_and(zz <= z, can_up))
                def _():
                    up(g, p).wait_send()

                @pl.when(jnp.logical_and(zz >= z, can_down))
                def _():
                    down(g, p).wait_send()

                across(g, p).wait_send()

        return carry

    lax.fori_loop(0, n_col, drain, 0)

    for j in range(1, n_col):
        got_lc(j).wait_recv()
    loss_out[...] = jnp.broadcast_to(
        jnp.sum(jnp.sum(loss_col[...], 0), keepdims=True) / width, loss_out.shape
    )
    for j in range(1, n_col):
        send_lc(j).wait_send()


def shards(view_a, view_b):
    t, width = view_a.shape
    n_row = lax.axis_size("row")
    n_col = lax.axis_size("col")
    rb = width // n_row
    cb = width // n_col
    count = t * n_row * n_col
    n_chunk = t * n_row
    dma = pltpu.SemaphoreType.DMA
    size = 2 * (count * (rb + cb) + 2 * n_chunk * cb + 2 * t * width) + 4 * rb * cb
    product, loss = pl.pallas_call(
        functools.partial(body, n_row, n_col, width),
        out_shape=(
            jax.ShapeDtypeStruct((rb, cb), F32),
            jax.ShapeDtypeStruct((8, 128), F32),
        ),
        in_specs=[pl.BlockSpec(memory_space=pltpu.HBM)] * 2,
        out_specs=(pl.BlockSpec(memory_space=pltpu.VMEM),) * 2,
        scratch_shapes=[
            pltpu.VMEM((n_col, n_chunk, rb), BF16),
            pltpu.VMEM((n_col, n_chunk, cb), BF16),
            pltpu.VMEM((2 * n_chunk, cb), BF16),
            pltpu.VMEM((n_col, 2, rb), F32),
            pltpu.VMEM((n_row, 2, cb), F32),
            pltpu.VMEM((2, rb), F32),
            pltpu.VMEM((2, cb), F32),
            pltpu.VMEM((n_row, 8, 128), F32),
            pltpu.VMEM((n_col, 8, 128), F32),
            dma((n_row,)), dma((n_row,)),
            dma((n_col,)), dma((n_col,)),
            dma((n_col,)), dma((n_col,)),
            dma((n_row,)), dma((n_row,)),
            dma((3, n_col, n_row)), dma((n_col, n_row)),
            dma((n_row, n_col)), dma((n_row, n_col)),
            dma((n_row,)), dma((n_row,)),
            dma((n_col,)), dma((n_col,)),
            dma((2,)),
        ],
        compiler_params=pltpu.CompilerParams(
            collective_id=0, has_side_effects=True, vmem_limit_bytes=min(size + (12 << 20), 60 << 20)
        ),
        name="twins",
    )(view_a, view_b)
    return product / count, loss[0, 0]


def solution(mesh):
    return jax.shard_map(
        shards,
        mesh=mesh,
        in_specs=(P(("row", "col"), None), P(("row", "col"), None)),
        out_specs=(P("row", "col"), P()),
        check_vma=False,
    )
```

```python
import functools

import jax
import jax.numpy as jnp
from jax import lax
from jax.experimental import pallas as pl
from jax.experimental.pallas import tpu as pltpu
from jax.sharding import PartitionSpec as P

MESH = pl.DeviceIdType.MESH
F32 = jnp.float32
BF16 = jnp.bfloat16


def body(
    n_row, n_col, width,
    a_in, b_in, out, loss_out,
    a_all, b_all, nb, stat_a, stat_b, coef_a, coef_b, loss_row, loss_col,
    s_a, r_a, s_b, r_b, s_sa, r_sa, s_sb, r_sb, s_line, r_line, s_fwd, r_fwd,
    s_lr, r_lr, s_lc, r_lc, own_sem,
):
    t = a_in.shape[0]
    rb = a_in.shape[1] // n_row
    cb = b_in.shape[1] // n_col
    count = t * n_row * n_col
    n_z = n_col // 2
    r = lax.axis_index("row")
    c = lax.axis_index("col")
    z = c // 2
    k = c % 2
    mine = pl.ds(pl.multiple_of(r * t, t), t)

    def row_mate(i):
        return (r + i) % n_row

    def col_mate(j):
        return (c + j) % n_col

    def remote(src, dst, ss, rs, dev):
        return pltpu.make_async_remote_copy(
            src_ref=src, dst_ref=dst, send_sem=ss, recv_sem=rs, device_id=dev, device_id_type=MESH
        )

    own_a = pltpu.make_async_copy(
        a_in.at[:, pl.ds(pl.multiple_of(r * rb, rb), rb)], a_all.at[c, mine], own_sem.at[0]
    )
    own_b = pltpu.make_async_copy(
        b_in.at[:, pl.ds(pl.multiple_of(c * cb, cb), cb)], b_all.at[c, mine], own_sem.at[1]
    )
    own_a.start()
    own_b.start()

    barrier = pltpu.get_barrier_semaphore()
    for i in range(1, n_row):
        pl.semaphore_signal(barrier, inc=1, device_id=(row_mate(i), c), device_id_type=MESH)
    for j in range(1, n_col):
        pl.semaphore_signal(barrier, inc=1, device_id=(r, col_mate(j)), device_id_type=MESH)
    pl.semaphore_wait(barrier, n_row + n_col - 2)

    def send_a(i):
        dst = row_mate(i)
        cols = pl.ds(pl.multiple_of(dst * rb, rb), rb)
        return remote(a_in.at[:, cols], a_all.at[c, mine], s_a.at[i], r_a.at[i], (dst, c))

    def got_a(i):
        src = row_mate(n_row - i)
        rows = pl.ds(pl.multiple_of(src * t, t), t)
        return remote(a_all.at[c, rows], a_all.at[c, rows], s_a.at[i], r_a.at[i], (src, c))

    def send_b(j):
        dst = col_mate(j)
        cols = pl.ds(pl.multiple_of(dst * cb, cb), cb)
        return remote(b_in.at[:, cols], b_all.at[c, mine], s_b.at[j], r_b.at[j], (r, dst))

    def got_b(j):
        src = col_mate(n_col - j)
        return remote(b_all.at[src, mine], b_all.at[src, mine], s_b.at[j], r_b.at[j], (r, src))

    for i in range(1, n_row):
        send_a(i).start()

    def line(way, chunk, p, dev_c):
        rows = pl.ds(pl.multiple_of(p * t, t), t)
        ref = a_all.at[chunk, rows]
        return remote(ref, ref, s_line.at[way, chunk, p], r_line.at[chunk, p], (r, dev_c))

    partner = z * 2 + (1 - k)

    def up(chunk, p):
        return line(0, chunk, p, lax.min(c + 2, n_col - 2 + k))

    def down(chunk, p):
        return line(1, chunk, p, lax.max(c - 2, k))

    def across(chunk, p):
        return line(2, chunk, p, partner)

    can_up = z < n_z - 1
    can_down = z > 0

    def slice_at(o):
        return (r + n_row - o) % n_row

    def send_line(o):
        p = slice_at(o)

        @pl.when(can_up)
        def _():
            up(c, p).start()

        @pl.when(can_down)
        def _():
            down(c, p).start()

        across(c, p).start()

    own_a.wait()
    send_line(0)

    for dist in range(n_z - 1, 0, -1):
        for side in range(2):
            zz = z - dist if side == 0 else z + dist

            @pl.when(jnp.logical_and(zz >= 0, zz < n_z))
            def _():
                for other in range(2):
                    send_b((zz * 2 + (k + other) % 2 + n_col - c) % n_col).start()

    send_b((partner + n_col - c) % n_col).start()

    for o in range(1, n_row):
        got_a(o).wait_recv()
        if o < n_row - 1:
            send_line(o)

    def moments_a(q, carry):
        cols = pl.ds(pl.multiple_of(q * 128, 128), 128)
        x = a_all[c, :, cols].astype(F32)
        stat_a[c, 0:1, cols] = jnp.sum(x, 0, keepdims=True)
        stat_a[c, 1:2, cols] = jnp.sum(x * x, 0, keepdims=True)
        return carry

    lax.fori_loop(0, rb // 128, moments_a, 0)

    def send_sa(j):
        return remote(stat_a.at[c], stat_a.at[c], s_sa.at[j], r_sa.at[j], (r, col_mate(j)))

    def got_sa(j):
        src = col_mate(n_col - j)
        return remote(stat_a.at[src], stat_a.at[src], s_sa.at[j], r_sa.at[j], (r, src))

    for j in range(1, n_col):
        send_sa(j).start()
    if n_row > 1:
        send_line(n_row - 1)

    def send_fwd(i, g):
        return remote(b_all.at[g, mine], b_all.at[g, mine], s_fwd.at[i, g], r_fwd.at[i, g], (row_mate(i), c))

    def got_fwd(i, g):
        src = row_mate(n_row - i)
        rows = pl.ds(pl.multiple_of(src * t, t), t)
        return remote(b_all.at[g, rows], b_all.at[g, rows], s_fwd.at[i, g], r_fwd.at[i, g], (src, c))

    def each_chunk(d, do):
        for side in range(2):
            zz = z - d if side == 0 else z + d
            ok = (zz >= 0) if side == 0 else jnp.logical_and(zz < n_z, d > 0)

            @pl.when(ok)
            def _():
                do(zz * 2 + k, side)
                do(zz * 2 + (1 - k), side)

    def forward(d, carry):
        def do(g, side):
            for i in range(1, n_row):
                send_fwd(i, g).start()

        each_chunk(d, do)
        return carry

    own_b.wait()
    near = 1 + (n_col - 2) * (1 - k)
    got_b(near).wait_recv()
    forward(0, 0)
    for j in range(1, n_col):
        @pl.when(j != near)
        def _():
            got_b(j).wait_recv()


    def moments_b(q, carry):
        cols = pl.ds(pl.multiple_of(q * 128, 128), 128)
        total = jnp.zeros((1, 128), F32)
        squares = jnp.zeros((1, 128), F32)
        for g in range(n_col):
            x = b_all[g, mine, cols].astype(F32)
            total = total + jnp.sum(x, 0, keepdims=True)
            squares = squares + jnp.sum(x * x, 0, keepdims=True)
        stat_b[r, 0:1, cols] = total
        stat_b[r, 1:2, cols] = squares
        return carry

    lax.fori_loop(0, cb // 128, moments_b, 0)

    def send_sb(i):
        return remote(stat_b.at[r], stat_b.at[r], s_sb.at[i], r_sb.at[i], (row_mate(i), c))

    def got_sb(i):
        src = row_mate(n_row - i)
        return remote(stat_b.at[src], stat_b.at[src], s_sb.at[i], r_sb.at[i], (src, c))

    for i in range(1, n_row):
        send_sb(i).start()

    lax.fori_loop(1, n_z, forward, 0)

    def clear(q, carry):
        rows = pl.ds(pl.multiple_of(q * 64, 64), 64)
        out[rows, :] = jnp.zeros((64, cb), F32)
        return carry

    lax.fori_loop(0, rb // 64, clear, 0)

    for j in range(1, n_col):
        got_sa(j).wait_recv()
    for i in range(1, n_row):
        got_sb(i).wait_recv()

    def coefs(stat, coef):
        sums = jnp.sum(stat[...], 0)
        mean = sums[0:1] / count
        var = sums[1:2] / count - mean * mean
        coef[0:1, :] = mean
        coef[1:2, :] = lax.rsqrt(var + 1e-05)

    coefs(stat_a, coef_a)
    coefs(stat_b, coef_b)

    tile = min(1024, rb)

    def wait_fwd(zz):
        for g in range(2):
            for i in range(1, n_row):
                got_fwd(i, zz * 2 + g).wait_recv()

    def process(zz):
        for p in range(n_row):
            across(zz * 2 + (1 - k), p).wait_recv()
        wait_fwd(zz)
        multiply(zz, pl.ds(0, n_row * t), n_row * t)

    def multiply(zz, rows, height):
        pair = pl.ds(zz * 2, 2)
        depth = 2 * height

        def norm_b(q, carry):
            cols = pl.ds(pl.multiple_of(q * 128, 128), 128)
            x = b_all[pair, rows, cols].astype(F32).reshape(depth, 128)
            nb[0:depth, cols] = ((x - coef_b[0:1, cols]) * coef_b[1:2, cols]).astype(BF16)
            return carry

        lax.fori_loop(0, cb // 128, norm_b, 0)

        def mul(q, carry):
            cols = pl.ds(pl.multiple_of(q * tile, tile), tile)
            x = a_all[pair, rows, cols].astype(F32).reshape(depth, tile)
            na = ((x - coef_a[0:1, cols]) * coef_a[1:2, cols]).astype(BF16)
            out[cols, :] += lax.dot_general(
                na, nb[0:depth, :], (((0,), (0,)), ((), ())), preferred_element_type=F32
            )
            return carry

        lax.fori_loop(0, rb // tile, mul, 0)

    def process_all(d):
        def one(side, carry):
            zz = jnp.where(side == 0, z - d, z + d)
            ok = jnp.logical_and(zz >= 0, zz < n_z)
            ok = jnp.logical_and(ok, jnp.logical_or(side == 0, d > 0))

            @pl.when(ok)
            def _():
                process(zz)

            return carry

        lax.fori_loop(0, 2, one, 0)

    def relay(d):
        from_low = z - d >= 0
        from_high = z + d < n_z
        low = (z - d) * 2 + k
        high = (z + d) * 2 + k
        for o in range(n_row):
            p = slice_at(o)

            @pl.when(from_low)
            def _():
                up(low, p).wait_recv()

                @pl.when(can_up)
                def _():
                    up(low, p).start()

                across(low, p).start()

            @pl.when(from_high)
            def _():
                down(high, p).wait_recv()

                @pl.when(can_down)
                def _():
                    down(high, p).start()

                across(high, p).start()

    def last():
        zz = jnp.where(z == 0, n_z - 1, 0)
        g = zz * 2 + k

        @pl.when(jnp.logical_or(z == 0, z == n_z - 1))
        def _():
            wait_fwd(zz)

            def one(o, carry):
                p = slice_at(o)
                up(g, p).wait_recv()
                across(g, p).start()
                across(zz * 2 + (1 - k), p).wait_recv()
                multiply(zz, pl.ds(pl.multiple_of(p * t, t), t), t)
                return carry

            lax.fori_loop(0, n_row, one, 0)

    def step(d, carry):
        @pl.when(d + 1 < n_z - 1)
        def _():
            relay(d + 1)

        process_all(d)

        return carry

    lax.fori_loop(0, max(n_z - 1, 1), step, 0)
    if n_z > 1:
        last()

    def part(q, carry):
        rows = pl.ds(pl.multiple_of(q * 8, 8), 8)
        x = out[rows, :] * (1.0 / count)
        row_ids = r * rb + q * 8 + lax.broadcasted_iota(jnp.int32, (8, cb), 0)
        col_ids = c * cb + lax.broadcasted_iota(jnp.int32, (8, cb), 1)
        sq = x * x
        return carry + jnp.where(row_ids == col_ids, (1.0 - x) * (1.0 - x), 0.0051 * sq)

    share = lax.fori_loop(0, rb // 8, part, jnp.zeros((8, cb), F32), unroll=4)
    folded = share[:, 0:128]
    for q in range(1, cb // 128):
        folded = folded + share[:, q * 128 : (q + 1) * 128]
    loss_row[r] = folded

    def send_lr(i):
        return remote(loss_row.at[r], loss_row.at[r], s_lr.at[i], r_lr.at[i], (row_mate(i), c))

    def got_lr(i):
        src = row_mate(n_row - i)
        return remote(loss_row.at[src], loss_row.at[src], s_lr.at[i], r_lr.at[i], (src, c))

    def send_lc(j):
        return remote(loss_col.at[c], loss_col.at[c], s_lc.at[j], r_lc.at[j], (r, col_mate(j)))

    def got_lc(j):
        src = col_mate(n_col - j)
        return remote(loss_col.at[src], loss_col.at[src], s_lc.at[j], r_lc.at[j], (r, src))

    for i in range(1, n_row):
        send_lr(i).start()
    for i in range(1, n_row):
        got_lr(i).wait_recv()
    loss_col[c] = jnp.sum(loss_row[...], 0)
    for j in range(1, n_col):
        send_lc(j).start()

    for i in range(1, n_row):
        send_a(i).wait_send()
        send_sb(i).wait_send()
        send_lr(i).wait_send()
    for j in range(1, n_col):
        send_b(j).wait_send()
        send_sa(j).wait_send()

    def drain(g, carry):
        for i in range(1, n_row):
            send_fwd(i, g).wait_send()
        zz = g // 2
        for p in range(n_row):
            @pl.when(g % 2 == k)
            def _():
                @pl.when(jnp.logical_and(zz <= z, can_up))
                def _():
                    up(g, p).wait_send()

                @pl.when(jnp.logical_and(zz >= z, can_down))
                def _():
                    down(g, p).wait_send()

                across(g, p).wait_send()

        return carry

    lax.fori_loop(0, n_col, drain, 0)

    for j in range(1, n_col):
        got_lc(j).wait_recv()
    loss_out[...] = jnp.broadcast_to(
        jnp.sum(jnp.sum(loss_col[...], 0), keepdims=True) / width, loss_out.shape
    )
    for j in range(1, n_col):
        send_lc(j).wait_send()


def shards(view_a, view_b):
    t, width = view_a.shape
    n_row = lax.axis_size("row")
    n_col = lax.axis_size("col")
    rb = width // n_row
    cb = width // n_col
    count = t * n_row * n_col
    n_chunk = t * n_row
    dma = pltpu.SemaphoreType.DMA
    size = 2 * (count * (rb + cb) + 2 * n_chunk * cb + 2 * t * width) + 4 * rb * cb
    product, loss = pl.pallas_call(
        functools.partial(body, n_row, n_col, width),
        out_shape=(
            jax.ShapeDtypeStruct((rb, cb), F32),
            jax.ShapeDtypeStruct((8, 128), F32),
        ),
        in_specs=[pl.BlockSpec(memory_space=pltpu.HBM)] * 2,
        out_specs=(pl.BlockSpec(memory_space=pltpu.VMEM),) * 2,
        scratch_shapes=[
            pltpu.VMEM((n_col, n_chunk, rb), BF16),
            pltpu.VMEM((n_col, n_chunk, cb), BF16),
            pltpu.VMEM((2 * n_chunk, cb), BF16),
            pltpu.VMEM((n_col, 2, rb), F32),
            pltpu.VMEM((n_row, 2, cb), F32),
            pltpu.VMEM((2, rb), F32),
            pltpu.VMEM((2, cb), F32),
            pltpu.VMEM((n_row, 8, 128), F32),
            pltpu.VMEM((n_col, 8, 128), F32),
            dma((n_row,)), dma((n_row,)),
            dma((n_col,)), dma((n_col,)),
            dma((n_col,)), dma((n_col,)),
            dma((n_row,)), dma((n_row,)),
            dma((3, n_col, n_row)), dma((n_col, n_row)),
            dma((n_row, n_col)), dma((n_row, n_col)),
            dma((n_row,)), dma((n_row,)),
            dma((n_col,)), dma((n_col,)),
            dma((2,)),
        ],
        compiler_params=pltpu.CompilerParams(
            collective_id=0, has_side_effects=True, vmem_limit_bytes=min(size + (12 << 20), 60 << 20)
        ),
        name="twins",
    )(view_a, view_b)
    return product / count, loss[0, 0]


def solution(mesh):
    return jax.shard_map(
        shards,
        mesh=mesh,
        in_specs=(P(("row", "col"), None), P(("row", "col"), None)),
        out_specs=(P("row", "col"), P()),
        check_vma=False,
    )
```
